16 devices in a mesh: rep: 2 (over y, z), dp: 8 (over x, core).
Axes of the slice: x: 4, y: 2, z: 1, core: 2. Of those that a mesh axis runs over, the one named last changes fastest.
The devices are a block of a 4x4x8 slice.
Arguments:
- x: bfloat16 [16, 2048, 768], P(('rep', 'dp')), parts along dimension 0
- dy: bfloat16 [16, 2048, 768], P(('rep', 'dp')), parts along dimension 0
- w_gate: bfloat16 [2, 768, 6144], P(None, 'dp')
- w_up: bfloat16 [2, 768, 6144], P(None, 'dp')
- w_down: bfloat16 [2, 6144, 768], P(None, 'dp')
- m_w_gate: float32 [2, 768, 6144], P(None, 'dp')
- m_w_up: float32 [2, 768, 6144], P(None, 'dp')
- m_w_down: float32 [2, 6144, 768], P(None, 'dp')
- v_w_gate: float32 [2, 768, 6144], P(None, 'dp')
- v_w_up: float32 [2, 768, 6144], P(None, 'dp')
- v_w_down: float32 [2, 6144, 768], P(None, 'dp')
Outputs:
- output 1: bfloat16 [4, 768, 6144], P('rep', 'dp'), parts along dimension 0
- output 2: bfloat16 [4, 768, 6144], P('rep', 'dp'), parts along dimension 0
- output 3: bfloat16 [4, 6144, 768], P('rep', 'dp'), parts along dimension 0
- output 4: float32 [4, 768, 6144], P('rep', 'dp'), parts along dimension 0
- output 5: float32 [4, 768, 6144], P('rep', 'dp'), parts along dimension 0
- output 6: float32 [4, 6144, 768], P('rep', 'dp'), parts along dimension 0
- output 7: float32 [4, 768, 6144], P('rep', 'dp'), parts along dimension 0
- output 8: float32 [4, 768, 6144], P('rep', 'dp'), parts along dimension 0
- output 9: float32 [4, 6144, 768], P('rep', 'dp'), parts along dimension 0
There are 2 independent parts. The reference program is written for one: setup_inputs(seed, part) draws one part's arguments, and reference() takes and returns one part's arrays. A program takes and returns all parts, laid end to end along the dimension named above; an argument that names none is the same for every part.
All inputs are finite; a program needn't handle non-finite values.
Results may differ from the reference program's by a relative error of at most 0.022.
Values are sent between devices in bfloat16 or wider.
A program may use at most 768 MiB of HBM per device.

```python
import jax
import jax.numpy as jnp
from jax import lax

SEQUENCES = 8
TOKENS = 2048
D = 768
FF = 6144
LAYERS = 2
NAMES = ("w_gate", "w_up", "w_down")
SHAPES = {"w_gate": (LAYERS, D, FF), "w_up": (LAYERS, D, FF), "w_down": (LAYERS, FF, D)}


def bump(key, n, height):
    away = (jnp.arange(n, dtype=jnp.int32) - jax.random.randint(key, (), 0, n, jnp.int32)) % n
    return jnp.where(away < n // 8, height, 1.0)


def together(key, own, strength):
    shared = jax.random.normal(key, own.shape[1:], jnp.float32)
    return (own + strength * shared) * lax.rsqrt(1 + strength * strength)


def setup_inputs(seed: int = 0, part: int = 0) -> dict:
    kx, kdy, ka, kb, kz, kf, kh, kl, *keys = jax.random.split(jax.random.key(seed), 8 + 3 * len(NAMES))
    kx, kdy, ka, kb = (jax.random.fold_in(k, part) for k in (kx, kdy, ka, kb))
    kw, km, kv = (keys[i::3] for i in range(3))
    shape = (SEQUENCES, TOKENS, D)
    much_x, much_dy = jax.random.uniform(kz, (2,), jnp.float32, 0.0, 1.0)
    loud = 2.0 ** jax.random.uniform(jax.random.fold_in(kz, 1), (), jnp.float32, -1.0, 2.0)
    layers = 2.0 ** jax.random.uniform(kl, (LAYERS, 1, 1), jnp.float32, -1.0, 1.0)
    x = together(ka, jax.random.normal(kx, shape, jnp.float32), much_x) * bump(kf, D, 4.0)
    dy = together(kb, jax.random.normal(kdy, shape, jnp.float32), much_dy)
    drawn = {"x": x.astype(jnp.bfloat16), "dy": (loud * dy * (SEQUENCES * TOKENS) ** -0.5).astype(jnp.bfloat16)}
    for key, name in zip(kw, NAMES, strict=True):
        w = jax.random.normal(key, SHAPES[name], jnp.float32) * SHAPES[name][1] ** -0.5
        drawn[name] = (w * {"w_gate": 1.0, "w_up": bump(kh, FF, 4.0), "w_down": layers}[name]).astype(jnp.bfloat16)
    for key, name in zip(km, NAMES, strict=True):
        drawn[f"m_{name}"] = 0.1 * jax.random.normal(key, SHAPES[name], jnp.float32)
    for key, name in zip(kv, NAMES, strict=True):
        drawn[f"v_{name}"] = jax.random.uniform(key, SHAPES[name], jnp.float32, 0.005, 0.015)
    return drawn


def matmul(a, w):
    return jnp.dot(a, w, preferred_element_type=jnp.float32).astype(jnp.bfloat16)


def normed(h):
    wide = h.astype(jnp.float32)
    scale = lax.rsqrt(jnp.mean(wide**2, -1, keepdims=True) + 1e-6)
    return (wide * scale).astype(jnp.bfloat16)


def layer(h, w):
    a = normed(h)
    gate = jnp.dot(a, w["w_gate"], preferred_element_type=jnp.float32)
    up = jnp.dot(a, w["w_up"], preferred_element_type=jnp.float32)
    return h + matmul((jax.nn.silu(gate) * up).astype(jnp.bfloat16), w["w_down"])


def adamw(w, m, v, g):
    m = 0.9 * m + 0.1 * g
    v = 0.95 * v + 0.05 * g * g
    step = m * lax.rsqrt(v + 1e-8) + 0.1 * w
    return (w - 0.02 * step).astype(jnp.bfloat16), m, v


def stack(weights, h):
    return lax.scan(lambda h, w: (layer(h, w), None), h, weights)[0]


def reference(x, dy, w_gate, w_up, w_down, m_w_gate, m_w_up, m_w_down, v_w_gate, v_w_up, v_w_down):
    weights = dict(zip(NAMES, (w_gate, w_up, w_down), strict=True))

    def take(so_far, sequence):
        h, by_y = sequence
        _, back = jax.vjp(lambda w: stack(w, h), weights)
        return jax.tree.map(lambda total, term: total + term.astype(jnp.float32), so_far, back(by_y)[0]), None

    none_yet = {name: jnp.zeros(w.shape, jnp.float32) for name, w in weights.items()}
    by_weights, _ = lax.scan(take, none_yet, (x, dy))
    gradients = [by_weights[name].astype(jnp.bfloat16).astype(jnp.float32) for name in NAMES]
    new = [
        adamw(w.astype(jnp.float32), m, v, g)
        for w, m, v, g in zip((w_gate, w_up, w_down), (m_w_gate, m_w_up, m_w_down), (v_w_gate, v_w_up, v_w_down), gradients, strict=True)
    ]
    return tuple(one[which] for which in range(3) for one in new)
```

```python
import functools

import jax
import jax.numpy as jnp
from jax import lax
from jax.experimental import pallas as pl
from jax.experimental.pallas import tpu as pltpu
from jax.sharding import PartitionSpec as P


BF16, F32 = jnp.bfloat16, jnp.float32
MESH = pl.DeviceIdType.MESH
NT, TN = ((1,), (1,)), ((0,), (0,))


def mm(a, w, dims):
    return lax.dot_general(a, w, (dims, ((), ())), preferred_element_type=F32)


def normed(h):
    wide = h.astype(F32)
    scale = lax.rsqrt(jnp.mean(wide**2, -1, keepdims=True) + 1e-6)
    return (wide * scale).astype(BF16)


def forward_kernel(n, x_ref, dy_ref, sg, su, sd, wg, wu, wd, keep_up, keep_gate, hid0, hid1, by_gate, by_up, h1, a1, a0, wd_v, send, recv, local, load):
    me = lax.axis_index("dp")
    chip, core = me // 2, lax.rem(me, 2)
    ring = n // 2
    at = lambda c, k: 2 * lax.rem(c, ring) + k
    right, left, partner = at(chip + 1, core), at(chip + ring - 1, core), at(chip, 1 - core)
    far = at(chip + 2, core)

    barrier = pltpu.get_barrier_semaphore()
    for other in (left, right, partner):
        pl.semaphore_signal(barrier, inc=1, device_id={"dp": other}, device_id_type=MESH)
    pl.semaphore_wait(barrier, 3)

    tokens, ff = hid0.shape
    d = x_ref.shape[1]
    third = ff // 3
    everything = (0, ff)
    units = [(sg, wg, 0, everything), (su, wu, 0, everything), (sd, wd, 0, (0, d)), (sd, wd, 1, (0, d))]
    for t in range(3):
        units += [(sg, wg, 1, (t * third, third)), (su, wu, 1, (t * third, third))]

    def span(u, part):
        depth = units[u][0].shape[1]
        half = depth // 2
        return {"all": (0, depth), "a": (0, half), "b": (half, half)}[part]

    def rows(u, owner, part):
        shard, full, layer, columns = units[u]
        start, size = span(u, part)
        return full.at[layer, pl.ds(pl.multiple_of(owner * shard.shape[1] + start, 16), size), pl.ds(*columns)]

    def own(u, part):
        shard, _, layer, columns = units[u]
        return shard.at[layer, pl.ds(*span(u, part)), pl.ds(*columns)]

    def move(u, kind):
        source, rows_of, to = [
            (own(u, "a"), (me, "a"), right),
            (own(u, "b"), (me, "b"), right),
            (own(u, "b"), (me, "b"), left),
            (own(u, "a"), (me, "a"), left),
            (None, (left, "a"), right),
            (None, (right, "b"), left),
            (own(u, "all"), (me, "all"), partner),
            (None, (left, "all"), partner),
            (None, (right, "all"), partner),
            (None, (far, "a"), partner),
            (None, (far, "b"), partner),
        ][kind]
        there = rows(u, *rows_of)
        return pltpu.make_async_remote_copy(
            src_ref=there if source is None else source,
            dst_ref=there,
            send_sem=send.at[u, kind],
            recv_sem=recv.at[u, kind],
            device_id={"dp": to},
            device_id_type=MESH,
        )

    def keep(u):
        return pltpu.make_async_copy(own(u, "all"), rows(u, me, "all"), local.at[u])

    def post(u):
        for kind in (0, 2, 1, 3, 6):
            move(u, kind).start()
        keep(u).start()

    def pass_on(arrived, onward):
        def act(u):
            for one, other in zip(arrived, onward):
                move(u, one).wait_recv()
                move(u, other).start()

        return act

    middle, relay, relay_far = pass_on((0, 2), (4, 5)), pass_on((1, 3), (7, 8)), pass_on((4, 5), (9, 10))

    def finish(u):
        for kind in (6, 7, 8, 9, 10):
            move(u, kind).wait_recv()
        keep(u).wait()

    def both(act, pair):
        act(4 + 2 * pair)
        act(5 + 2 * pair)

    bn, sub = 256, 256

    def when(step, plan):
        for number, act in plan.items():
            pl.when(step == number)(act)

    def first_layer(plan):
        def body(g_ref, u_ref, ku_ref, kg_ref, h_ref):
            when(pl.program_id(0), plan)
            for r in range(0, tokens, sub):
                here = pl.ds(r, sub)
                gate = jnp.dot(a0[here, :], g_ref[...], preferred_element_type=F32)
                up = jnp.dot(a0[here, :], u_ref[...], preferred_element_type=F32)
                sig = 0.5 * jnp.tanh(0.5 * gate) + 0.5
                silu = gate * sig
                ku_ref[here, :] = silu
                kg_ref[here, :] = up * (sig + silu * (1 - sig))
                h_ref[here, :] = (silu * up).astype(BF16)

        w, tile = pl.BlockSpec((d, bn), lambda j: (0, j)), pl.BlockSpec((tokens, bn), lambda j: (0, j))
        pltpu.emit_pipeline(body, grid=(ff // bn,), in_specs=[w, w], out_specs=[tile] * 3)(
            wg.at[0], wu.at[0], keep_up, keep_gate, hid0
        )

    def last_layer(part, plan):
        steps = third // bn

        def body(g_ref, u_ref, d_ref, h_ref, bg_ref, bu_ref):
            when(pl.program_id(0), plan)
            for r in range(0, tokens, sub):
                here = pl.ds(r, sub)
                gate = jnp.dot(a1[here, :], g_ref[...], preferred_element_type=F32)
                up = jnp.dot(a1[here, :], u_ref[...], preferred_element_type=F32)
                by = mm(dy_ref[here, :], d_ref[...], NT).astype(BF16).astype(F32)
                sig = 0.5 * jnp.tanh(0.5 * gate) + 0.5
                silu = gate * sig
                h_ref[here, :] = (silu * up).astype(BF16)
                bu_ref[here, :] = (by * silu).astype(BF16)
                bg_ref[here, :] = (by * (up * (sig + silu * (1 - sig)))).astype(BF16)

        w = pl.BlockSpec((d, bn), lambda j: (0, part * steps + j))
        wt = pl.BlockSpec((bn, d), lambda j: (part * steps + j, 0))
        tile = pl.BlockSpec((tokens, bn), lambda j: (0, part * steps + j))
        pltpu.emit_pipeline(body, grid=(steps,), in_specs=[w, w, wt], out_specs=[tile] * 3)(
            wg.at[1], wu.at[1], wd.at[1], hid1, by_gate, by_up
        )

    rm = 256

    def down(plan):
        def body(hid_ref):
            i = pl.program_id(0)
            when(i, plan)
            here = pl.ds(pl.multiple_of(i * rm, rm), rm)
            out = jnp.dot(hid_ref[...], wd_v[...], preferred_element_type=F32).astype(BF16)
            h = (x_ref[here, :].astype(F32) + out.astype(F32)).astype(BF16)
            h1[here, :] = h
            a1[here, :] = normed(h)

        pltpu.emit_pipeline(body, grid=(tokens // rm,), in_specs=[pl.BlockSpec((rm, ff), lambda i: (i, 0))], out_specs=[])(hid0)

    def run(*acts):
        def act():
            for f, u in acts:
                f(u)

        return act

    post(0)
    post(1)

    @pl.loop(0, tokens // rm)
    def _(i):
        here = pl.ds(pl.multiple_of(i * rm, rm), rm)
        a0[here, :] = normed(x_ref[here, :])

    run((middle, 0), (relay, 0), (middle, 1), (post, 2), (relay, 1), (relay_far, 0), (relay_far, 1), (post, 3), (finish, 0), (finish, 1))()
    pair = lambda p: lambda act: lambda: both(act, p)
    p0, p1, p2 = pair(0), pair(1), pair(2)
    first_layer(
        {
            6: run((middle, 2)),
            11: run((relay, 2)),
            12: p0(post),
            16: run((middle, 3)),
            21: run((relay, 3)),
        }
    )
    run((relay_far, 2), (finish, 2))()
    get = pltpu.make_async_copy(wd.at[0], wd_v, load)
    get.start()
    get.wait()

    def after_first():
        p0(middle)()
        p1(post)()

    down({3: after_first, 6: p0(relay)})
    run((relay_far, 3), (finish, 3))()
    p0(relay_far)()
    p0(finish)()

    def after_second():
        p1(middle)()
        p2(post)()

    last_layer(0, {2: after_second, 5: p1(relay)})
    p1(relay_far)()
    p1(finish)()
    last_layer(1, {2: p2(middle), 5: p2(relay)})
    p2(relay_far)()
    p2(finish)()
    last_layer(2, {})
    for u in range(len(units)):
        for kind in range(11):
            move(u, kind).wait_send()


def forward(n, x, dy, sg, su, sd):
    tokens, d = x.shape
    ff = sg.shape[-1]
    layers = sg.shape[0]
    vmem, hbm = pl.BlockSpec(memory_space=pltpu.VMEM), pl.BlockSpec(memory_space=pl.ANY)
    s = jax.ShapeDtypeStruct
    wide, thin = s((tokens, ff), F32), s((tokens, ff), BF16)
    units, kinds = 10, 11
    return pl.pallas_call(
        functools.partial(forward_kernel, n),
        out_shape=(
            s((layers, d, ff), BF16), s((layers, d, ff), BF16), s((layers, ff, d), BF16),
            wide, wide, thin, thin, thin, thin, s((tokens, d), BF16), s((tokens, d), BF16),
        ),
        in_specs=[vmem] * 5,
        out_specs=[hbm] * 9 + [vmem] * 2,
        scratch_shapes=[
            pltpu.VMEM((tokens, d), BF16),
            pltpu.VMEM((ff, d), BF16),
            pltpu.SemaphoreType.DMA((units, kinds)),
            pltpu.SemaphoreType.DMA((units, kinds)),
            pltpu.SemaphoreType.DMA((units,)),
            pltpu.SemaphoreType.DMA,
        ],
        compiler_params=pltpu.CompilerParams(collective_id=0, has_side_effects=True, vmem_limit_bytes=63 * 1024 * 1024),
        name="forward",
    )(x, dy, sg, su, sd)


def normed_back(h, by_a):
    wide, by = h.astype(F32), by_a.astype(F32)
    scale = lax.rsqrt(jnp.mean(wide**2, -1, keepdims=True) + 1e-6)
    along = jnp.mean(by * wide, -1, keepdims=True)
    return (by * scale - scale**3 * along * wide).astype(BF16)


def adamw(w, m, v, g):
    m = 0.9 * m + 0.1 * g
    v = 0.95 * v + 0.05 * g * g
    step = m * lax.rsqrt(v + 1e-8) + 0.1 * w
    return (w - 0.02 * step).astype(BF16), m, v


def solution(mesh):
    n = mesh.shape["dp"]

    def scatter(g):
        return lax.psum_scatter(g, "dp", scatter_dimension=0, tiled=True)

    def inner(x, dy, *arrays):
        weights, m, v = (arrays[i : i + 3] for i in (0, 3, 6))
        layers = weights[0].shape[0]
        wg, wu, wd, keep_up, keep_gate, hid0, hid1, by_gate, by_up, h1, a1 = forward(n, x[0], dy[0], *weights)
        a0, by_h = normed(x[0]), dy[0]
        g_down = mm(hid1, by_h, TN).astype(BF16)
        r0 = scatter(g_down)
        by_gate, by_up, g_down = lax.optimization_barrier((by_gate, by_up, g_down))
        g_gate = mm(a1, by_gate, TN).astype(BF16)
        r1 = scatter(g_gate)
        by_up, g_gate = lax.optimization_barrier((by_up, g_gate))
        g_up = mm(a1, by_up, TN).astype(BF16)
        r2 = scatter(g_up)
        by_gate, by_up, g_up = lax.optimization_barrier((by_gate, by_up, g_up))
        by_a = mm(by_gate, wg[1], NT).astype(BF16) + mm(by_up, wu[1], NT).astype(BF16)
        by_h = by_h + normed_back(h1, by_a)
        g_down = mm(hid0, by_h, TN).astype(BF16)
        r3 = scatter(g_down)
        by_h, g_down = lax.optimization_barrier((by_h, g_down))
        by_hidden = mm(by_h, wd[0], NT).astype(BF16).astype(F32)
        by_up, by_gate = (by_hidden * keep_up).astype(BF16), (by_hidden * keep_gate).astype(BF16)
        by_gate, by_up = lax.optimization_barrier((by_gate, by_up))
        g_gate = mm(a0, by_gate, TN).astype(BF16)
        r4 = scatter(g_gate)
        by_up, g_gate = lax.optimization_barrier((by_up, g_gate))
        r5 = scatter(mm(a0, by_up, TN).astype(BF16))
        mine = [[r4, r5, r3], [r1, r2, r0]]
        new = []
        for i in range(3):
            g = jnp.stack([mine[layer][i] for layer in range(layers)]).astype(F32)
            new.append(adamw(weights[i].astype(F32), m[i], v[i], g))
        return tuple(one[which] for which in range(3) for one in new)

    states, cut = P(("rep", "dp"), None, None), P(None, "dp", None)
    return jax.shard_map(
        inner,
        mesh=mesh,
        in_specs=(states, states) + (cut,) * 9,
        out_specs=(P("rep", "dp", None),) * 9,
        check_vma=False,
    )
```

```python
import functools

import jax
import jax.numpy as jnp
from jax import lax
from jax.experimental import pallas as pl
from jax.experimental.pallas import tpu as pltpu
from jax.sharding import PartitionSpec as P


BF16, F32 = jnp.bfloat16, jnp.float32
MESH = pl.DeviceIdType.MESH
NT, TN = ((1,), (1,)), ((0,), (0,))


def mm(a, w, dims):
    return lax.dot_general(a, w, (dims, ((), ())), preferred_element_type=F32)


def normed(h):
    wide = h.astype(F32)
    scale = lax.rsqrt(jnp.mean(wide**2, -1, keepdims=True) + 1e-6)
    return (wide * scale).astype(BF16)


def forward_kernel(n, x_ref, dy_ref, sg, su, sd, wg, wu, wd, keep_up, keep_gate, hid0, hid1, by_gate, by_up, h1, a1, a0, wd_v, send, recv, local, load):
    me = lax.axis_index("dp")
    chip, core = me // 2, lax.rem(me, 2)
    ring = n // 2
    at = lambda c, k: 2 * lax.rem(c, ring) + k
    right, left, partner = at(chip + 1, core), at(chip + ring - 1, core), at(chip, 1 - core)
    far = at(chip + 2, core)

    barrier = pltpu.get_barrier_semaphore()
    for other in (left, right, partner):
        pl.semaphore_signal(barrier, inc=1, device_id={"dp": other}, device_id_type=MESH)
    pl.semaphore_wait(barrier, 3)

    tokens, ff = hid0.shape
    d = x_ref.shape[1]
    third = ff // 3
    everything = (0, ff)
    units = [(sg, wg, 0, everything), (su, wu, 0, everything), (sd, wd, 0, (0, d)), (sd, wd, 1, (0, d))]
    for t in range(3):
        units += [(sg, wg, 1, (t * third, third)), (su, wu, 1, (t * third, third))]

    def span(u, part):
        depth = units[u][0].shape[1]
        half = depth // 2
        return {"all": (0, depth), "a": (0, half), "b": (half, half)}[part]

    def rows(u, owner, part):
        shard, full, layer, columns = units[u]
        start, size = span(u, part)
        return full.at[layer, pl.ds(pl.multiple_of(owner * shard.shape[1] + start, 16), size), pl.ds(*columns)]

    def own(u, part):
        shard, _, layer, columns = units[u]
        return shard.at[layer, pl.ds(*span(u, part)), pl.ds(*columns)]

    def move(u, kind):
        source, rows_of, to = [
            (own(u, "a"), (me, "a"), right),
            (own(u, "b"), (me, "b"), right),
            (own(u, "b"), (me, "b"), left),
            (own(u, "a"), (me, "a"), left),
            (None, (left, "a"), right),
            (None, (right, "b"), left),
            (own(u, "all"), (me, "all"), partner),
            (None, (left, "all"), partner),
            (None, (right, "all"), partner),
            (None, (far, "a"), partner),
            (None, (far, "b"), partner),
        ][kind]
        there = rows(u, *rows_of)
        return pltpu.make_async_remote_copy(
            src_ref=there if source is None else source,
            dst_ref=there,
            send_sem=send.at[u, kind],
            recv_sem=recv.at[u, kind],
            device_id={"dp": to},
            device_id_type=MESH,
        )

    def keep(u):
        return pltpu.make_async_copy(own(u, "all"), rows(u, me, "all"), local.at[u])

    def post(u):
        for kind in (0, 2, 1, 3, 6):
            move(u, kind).start()
        keep(u).start()

    def pass_on(arrived, onward):
        def act(u):
            for one, other in zip(arrived, onward):
                move(u, one).wait_recv()
                move(u, other).start()

        return act

    middle, relay, relay_far = pass_on((0, 2), (4, 5)), pass_on((1, 3), (7, 8)), pass_on((4, 5), (9, 10))

    def finish(u):
        for kind in (6, 7, 8, 9, 10):
            move(u, kind).wait_recv()
        keep(u).wait()

    def both(act, pair):
        act(4 + 2 * pair)
        act(5 + 2 * pair)

    bn, sub = 256, 256

    def when(step, plan):
        for number, act in plan.items():
            pl.when(step == number)(act)

    def first_layer(plan):
        def body(g_ref, u_ref, ku_ref, kg_ref, h_ref):
            when(pl.program_id(0), plan)
            for r in range(0, tokens, sub):
                here = pl.ds(r, sub)
                gate = jnp.dot(a0[here, :], g_ref[...], preferred_element_type=F32)
                up = jnp.dot(a0[here, :], u_ref[...], preferred_element_type=F32)
                sig = 0.5 * jnp.tanh(0.5 * gate) + 0.5
                silu = gate * sig
                ku_ref[here, :] = silu
                kg_ref[here, :] = up * (sig + silu * (1 - sig))
                h_ref[here, :] = (silu * up).astype(BF16)

        w, tile = pl.BlockSpec((d, bn), lambda j: (0, j)), pl.BlockSpec((tokens, bn), lambda j: (0, j))
        pltpu.emit_pipeline(body, grid=(ff // bn,), in_specs=[w, w], out_specs=[tile] * 3)(
            wg.at[0], wu.at[0], keep_up, keep_gate, hid0
        )

    def last_layer(part, plan):
        steps = third // bn

        def body(g_ref, u_ref, d_ref, h_ref, bg_ref, bu_ref):
            when(pl.program_id(0), plan)
            for r in range(0, tokens, sub):
                here = pl.ds(r, sub)
                gate = jnp.dot(a1[here, :], g_ref[...], preferred_element_type=F32)
                up = jnp.dot(a1[here, :], u_ref[...], preferred_element_type=F32)
                by = mm(dy_ref[here, :], d_ref[...], NT).astype(BF16).astype(F32)
                sig = 0.5 * jnp.tanh(0.5 * gate) + 0.5
                silu = gate * sig
                h_ref[here, :] = (silu * up).astype(BF16)
                bu_ref[here, :] = (by * silu).astype(BF16)
                bg_ref[here, :] = (by * (up * (sig + silu * (1 - sig)))).astype(BF16)

        w = pl.BlockSpec((d, bn), lambda j: (0, part * steps + j))
        wt = pl.BlockSpec((bn, d), lambda j: (part * steps + j, 0))
        tile = pl.BlockSpec((tokens, bn), lambda j: (0, part * steps + j))
        pltpu.emit_pipeline(body, grid=(steps,), in_specs=[w, w, wt], out_specs=[tile] * 3)(
            wg.at[1], wu.at[1], wd.at[1], hid1, by_gate, by_up
        )

    rm = 256

    def down(plan):
        def body(hid_ref):
            i = pl.program_id(0)
            when(i, plan)
            here = pl.ds(pl.multiple_of(i * rm, rm), rm)
            out = jnp.dot(hid_ref[...], wd_v[...], preferred_element_type=F32).astype(BF16)
            h = (x_ref[here, :].astype(F32) + out.astype(F32)).astype(BF16)
            h1[here, :] = h
            a1[here, :] = normed(h)

        pltpu.emit_pipeline(body, grid=(tokens // rm,), in_specs=[pl.BlockSpec((rm, ff), lambda i: (i, 0))], out_specs=[])(hid0)

    def run(*acts):
        def act():
            for f, u in acts:
                f(u)

        return act

    post(0)
    post(1)

    @pl.loop(0, tokens // rm)
    def _(i):
        here = pl.ds(pl.multiple_of(i * rm, rm), rm)
        a0[here, :] = normed(x_ref[here, :])

    run((middle, 0), (relay, 0), (middle, 1), (post, 2), (relay, 1), (relay_far, 0), (relay_far, 1), (post, 3), (finish, 0), (finish, 1))()
    pair = lambda p: lambda act: lambda: both(act, p)
    p0, p1, p2 = pair(0), pair(1), pair(2)
    first_layer(
        {
            6: run((middle, 2)),
            11: run((relay, 2)),
            12: p0(post),
            16: run((middle, 3)),
            21: run((relay, 3)),
        }
    )
    run((relay_far, 2), (finish, 2))()
    get = pltpu.make_async_copy(wd.at[0], wd_v, load)
    get.start()
    get.wait()

    def after_first():
        p0(middle)()
        p1(post)()

    down({3: after_first, 6: p0(relay)})
    run((relay_far, 3), (finish, 3))()
    p0(relay_far)()
    p0(finish)()

    def after_second():
        p1(middle)()
        p2(post)()

    last_layer(0, {2: after_second, 5: p1(relay)})
    p1(relay_far)()
    p1(finish)()
    last_layer(1, {2: p2(middle), 5: p2(relay)})
    p2(relay_far)()
    p2(finish)()
    last_layer(2, {})
    for u in range(len(units)):
        for kind in range(11):
            move(u, kind).wait_send()


def forward(n, x, dy, sg, su, sd):
    tokens, d = x.shape
    ff = sg.shape[-1]
    layers = sg.shape[0]
    vmem, hbm = pl.BlockSpec(memory_space=pltpu.VMEM), pl.BlockSpec(memory_space=pl.ANY)
    s = jax.ShapeDtypeStruct
    wide, thin = s((tokens, ff), F32), s((tokens, ff), BF16)
    units, kinds = 10, 11
    return pl.pallas_call(
        functools.partial(forward_kernel, n),
        out_shape=(
            s((layers, d, ff), BF16), s((layers, d, ff), BF16), s((layers, ff, d), BF16),
            wide, wide, thin, thin, thin, thin, s((tokens, d), BF16), s((tokens, d), BF16),
        ),
        in_specs=[vmem] * 5,
        out_specs=[hbm] * 9 + [vmem] * 2,
        scratch_shapes=[
            pltpu.VMEM((tokens, d), BF16),
            pltpu.VMEM((ff, d), BF16),
            pltpu.SemaphoreType.DMA((units, kinds)),
            pltpu.SemaphoreType.DMA((units, kinds)),
            pltpu.SemaphoreType.DMA((units,)),
            pltpu.SemaphoreType.DMA,
        ],
        compiler_params=pltpu.CompilerParams(collective_id=0, has_side_effects=True, vmem_limit_bytes=63 * 1024 * 1024),
        name="forward",
    )(x, dy, sg, su, sd)


def tail_kernel(n, by_ref, at_ref, wd, keep_up, keep_gate, out, bg, bu, term, there, own, hold, first, second, far_a, far_b, low, high, send, recv):
    me = lax.axis_index("dp")
    chip, core = me // 2, lax.rem(me, 2)
    ring = n // 2
    at = lambda c, k: 2 * lax.rem(c, ring) + k
    right, left, partner = at(chip + 1, core), at(chip + ring - 1, core), at(chip, 1 - core)

    barrier = pltpu.get_barrier_semaphore()
    for other in (left, right, partner):
        pl.semaphore_signal(barrier, inc=1, device_id={"dp": other}, device_id_type=MESH)
    pl.semaphore_wait(barrier, 3)

    tokens, d = by_ref.shape
    slices, bn = there.shape[0], there.shape[-1]
    slots = hold.shape[0]

    def move(u, kind):
        slot = lax.rem(u, slots)
        source, target, to = [
            (term.at[lax.rem(u, 2), :, :, 1 - core], there.at[u], partner),
            (first.at[slot, 0], far_a.at[u], right),
            (first.at[slot, 1], far_b.at[u], left),
            (first.at[slot, 2], low.at[u, 1], right),
            (first.at[slot, 3], high.at[u, 0], left),
            (second.at[slot, 0], low.at[u, 0], right),
            (second.at[slot, 1], high.at[u, 1], left),
        ][kind]
        return pltpu.make_async_remote_copy(
            src_ref=source, dst_ref=target, send_sem=send.at[u, kind], recv_sem=recv.at[u, kind], device_id={"dp": to}, device_id_type=MESH
        )

    def pair_sum(u):
        slot, turn = lax.rem(u, slots), lax.rem(u, 2)
        move(u, 0).wait_recv()

        @pl.when(u >= slots)
        def _():
            for kind in (1, 2, 3, 4):
                move(u - slots, kind).wait_send()

        def both(away, which):
            c = lax.rem(chip + away, ring)
            return term[turn, which, c, core].astype(F32) + there[u, which, c].astype(F32)

        for i, (away, which) in enumerate(((2, 0), (2, 1), (1, 1), (ring - 1, 0))):
            first[slot, i] = both(away, which).astype(BF16)
        for kind in (1, 2, 3, 4):
            move(u, kind).start()
        hold[slot, 0] = both(1, 0)
        hold[slot, 1] = both(ring - 1, 1)
        for which in range(2):
            own[u, which] = both(0, which)

    def add_far(u):
        slot = lax.rem(u, slots)

        @pl.when(u >= slots)
        def _():
            for kind in (5, 6):
                move(u - slots, kind).wait_send()

        for i, far in enumerate((far_a, far_b)):
            move(u, 1 + i).wait_recv()
            second[slot, i] = (hold[slot, i] + far[u].astype(F32)).astype(BF16)
            move(u, 5 + i).start()

    def finish(u):
        for kind in (3, 4, 5, 6):
            move(u, kind).wait_recv()
        columns = pl.ds(pl.multiple_of(u * bn, bn), bn)
        for which in range(2):
            total = own[u, which] + low[u, which].astype(F32) + high[u, which].astype(F32)
            out[which, :, columns] = total.astype(BF16)

    bm, sub = tokens // 2, 256

    def body(d_ref, ku_ref, kg_ref):
        j, i = pl.program_id(0), pl.program_id(1)

        @pl.when((i == 0) & (j >= 3))
        def _():
            finish(j - 3)

        @pl.when((i == 0) & (j >= 2))
        def _():
            add_far(j - 2)

        for r in range(0, bm, sub):
            here, whole = pl.ds(r, sub), pl.ds(pl.multiple_of(i * bm + r, sub), sub)
            by = mm(by_ref[whole, :], d_ref[...], NT).astype(BF16).astype(F32)
            bu[whole, :] = (by * ku_ref[here, :]).astype(BF16)
            bg[whole, :] = (by * kg_ref[here, :]).astype(BF16)

        @pl.when((i == 0) & (j >= 1))
        def _():
            pair_sum(j - 1)

        @pl.when(i == 1)
        def _():
            @pl.when(j >= 2)
            def _():
                move(j - 2, 0).wait_send()

            for which, by in enumerate((bg, bu)):
                g = jnp.dot(at_ref[...], by[...], preferred_element_type=F32).astype(BF16)
                term[lax.rem(j, 2), which] = g.reshape(term.shape[2:])
            move(j, 0).start()

    tile = pl.BlockSpec((bm, bn), lambda j, i: (i, j))
    pltpu.emit_pipeline(
        body, grid=(slices, 2), in_specs=[pl.BlockSpec((bn, d), lambda j, i: (j, 0)), tile, tile], out_specs=[]
    )(wd.at[0], keep_up, keep_gate)

    finish(slices - 3)
    add_far(slices - 2)
    pair_sum(slices - 1)
    finish(slices - 2)
    add_far(slices - 1)
    finish(slices - 1)
    for u in range(slices - 2, slices):
        move(u, 0).wait_send()
    for u in range(slices - slots, slices):
        for kind in range(1, 7):
            move(u, kind).wait_send()


def tail(n, by_h, a, wd, keep_up, keep_gate):
    tokens, d = by_h.shape
    ff = keep_up.shape[1]
    depth, bn = d // n, 512
    slices, slots, ring = ff // bn, 4, n // 2
    vmem, hbm = pl.BlockSpec(memory_space=pltpu.VMEM), pl.BlockSpec(memory_space=pl.ANY)
    block = (depth, bn)
    return pl.pallas_call(
        functools.partial(tail_kernel, n),
        out_shape=jax.ShapeDtypeStruct((2, depth, ff), BF16),
        in_specs=[vmem, vmem, hbm, hbm, hbm],
        out_specs=vmem,
        scratch_shapes=[
            pltpu.VMEM((tokens, bn), BF16),
            pltpu.VMEM((tokens, bn), BF16),
            pltpu.VMEM((2, 2, ring, 2) + block, BF16),
            pltpu.VMEM((slices, 2, ring) + block, BF16),
            pltpu.VMEM((slices, 2) + block, F32),
            pltpu.VMEM((slots, 2) + block, F32),
            pltpu.VMEM((slots, 4) + block, BF16),
            pltpu.VMEM((slots, 2) + block, BF16),
            pltpu.VMEM((slices,) + block, BF16),
            pltpu.VMEM((slices,) + block, BF16),
            pltpu.VMEM((slices, 2) + block, BF16),
            pltpu.VMEM((slices, 2) + block, BF16),
            pltpu.SemaphoreType.DMA((slices, 7)),
            pltpu.SemaphoreType.DMA((slices, 7)),
        ],
        compiler_params=pltpu.CompilerParams(collective_id=1, has_side_effects=True, vmem_limit_bytes=63 * 1024 * 1024),
        name="tail",
    )(by_h, a.T, wd, keep_up, keep_gate)


def normed_back(h, by_a):
    wide, by = h.astype(F32), by_a.astype(F32)
    scale = lax.rsqrt(jnp.mean(wide**2, -1, keepdims=True) + 1e-6)
    along = jnp.mean(by * wide, -1, keepdims=True)
    return (by * scale - scale**3 * along * wide).astype(BF16)


def adamw(w, m, v, g):
    m = 0.9 * m + 0.1 * g
    v = 0.95 * v + 0.05 * g * g
    step = m * lax.rsqrt(v + 1e-8) + 0.1 * w
    return (w - 0.02 * step).astype(BF16), m, v


def solution(mesh):
    n = mesh.shape["dp"]

    def scatter(g):
        return lax.psum_scatter(g, "dp", scatter_dimension=0, tiled=True)

    def inner(x, dy, *arrays):
        weights, m, v = (arrays[i : i + 3] for i in (0, 3, 6))
        layers = weights[0].shape[0]
        wg, wu, wd, keep_up, keep_gate, hid0, hid1, by_gate, by_up, h1, a1 = forward(n, x[0], dy[0], *weights)
        a0, by_h = normed(x[0]), dy[0]
        g_down = mm(hid1, by_h, TN).astype(BF16)
        r0 = scatter(g_down)
        by_gate, by_up, g_down = lax.optimization_barrier((by_gate, by_up, g_down))
        g_gate = mm(a1, by_gate, TN).astype(BF16)
        r1 = scatter(g_gate)
        by_up, g_gate = lax.optimization_barrier((by_up, g_gate))
        g_up = mm(a1, by_up, TN).astype(BF16)
        r2 = scatter(g_up)
        by_gate, by_up, g_up = lax.optimization_barrier((by_gate, by_up, g_up))
        by_a = mm(by_gate, wg[1], NT).astype(BF16) + mm(by_up, wu[1], NT).astype(BF16)
        by_h = by_h + normed_back(h1, by_a)
        g_down = mm(hid0, by_h, TN).astype(BF16)
        r3 = scatter(g_down)
        by_h, g_down = lax.optimization_barrier((by_h, g_down))
        r4, r5 = tail(n, by_h, a0, wd, keep_up, keep_gate)
        mine = [[r4, r5, r3], [r1, r2, r0]]
        new = []
        for i in range(3):
            g = jnp.stack([mine[layer][i] for layer in range(layers)]).astype(F32)
            new.append(adamw(weights[i].astype(F32), m[i], v[i], g))
        return tuple(one[which] for which in range(3) for one in new)

    states, cut = P(("rep", "dp"), None, None), P(None, "dp", None)
    return jax.shard_map(
        inner,
        mesh=mesh,
        in_specs=(states, states) + (cut,) * 9,
        out_specs=(P("rep", "dp", None),) * 9,
        check_vma=False,
    )
```

```python
import functools

import jax
import jax.numpy as jnp
from jax import lax
from jax.experimental import pallas as pl
from jax.experimental.pallas import tpu as pltpu
from jax.sharding import PartitionSpec as P


BF16, F32 = jnp.bfloat16, jnp.float32
MESH = pl.DeviceIdType.MESH
NT, TN = ((1,), (1,)), ((0,), (0,))


def mm(a, w, dims):
    return lax.dot_general(a, w, (dims, ((), ())), preferred_element_type=F32)


def normed(h):
    wide = h.astype(F32)
    scale = lax.rsqrt(jnp.mean(wide**2, -1, keepdims=True) + 1e-6)
    return (wide * scale).astype(BF16)


def normed_back(h, by_a):
    wide, by = h.astype(F32), by_a.astype(F32)
    scale = lax.rsqrt(jnp.mean(wide**2, -1, keepdims=True) + 1e-6)
    along = jnp.mean(by * wide, -1, keepdims=True)
    return (by * scale - scale**3 * along * wide).astype(BF16)


def forward_kernel(n, x_ref, dy, sg, su, sd, wg, wu, wd, keep_up, keep_gate, hid0, hid1, by_gate, by_up, h1_out, a1t_out, a0t_out, h1, a1t, a0t, a0, a1, dy_ref, wd_v, send, recv, local, load, leave):
    me = lax.axis_index("dp")
    chip, core = me // 2, lax.rem(me, 2)
    ring = n // 2
    at = lambda c, k: 2 * lax.rem(c, ring) + k
    right, left, partner = at(chip + 1, core), at(chip + ring - 1, core), at(chip, 1 - core)
    far = at(chip + 2, core)

    barrier = pltpu.get_barrier_semaphore()
    for other in (left, right, partner):
        pl.semaphore_signal(barrier, inc=1, device_id={"dp": other}, device_id_type=MESH)
    pl.semaphore_wait(barrier, 3)

    tokens, ff = hid0.shape
    d = x_ref.shape[1]
    pieces = 6
    piece = ff // pieces
    everything = (0, ff)
    units = [(sg, wg, 0, everything), (su, wu, 0, everything), (sd, wd, 0, (0, d)), (sd, wd, 1, (0, d))]
    for t in range(pieces):
        units += [(sg, wg, 1, (t * piece, piece)), (su, wu, 1, (t * piece, piece))]

    def span(u, part):
        depth = units[u][0].shape[1]
        half = depth // 2
        return {"all": (0, depth), "a": (0, half), "b": (half, half)}[part]

    def rows(u, owner, part):
        shard, full, layer, columns = units[u]
        start, size = span(u, part)
        return full.at[layer, pl.ds(pl.multiple_of(owner * shard.shape[1] + start, 16), size), pl.ds(*columns)]

    def own(u, part):
        shard, _, layer, columns = units[u]
        return shard.at[layer, pl.ds(*span(u, part)), pl.ds(*columns)]

    def move(u, kind):
        source, rows_of, to = [
            (own(u, "a"), (me, "a"), right),
            (own(u, "b"), (me, "b"), right),
            (own(u, "b"), (me, "b"), left),
            (own(u, "a"), (me, "a"), left),
            (None, (left, "a"), right),
            (None, (right, "b"), left),
            (own(u, "all"), (me, "all"), partner),
            (None, (left, "all"), partner),
            (None, (right, "all"), partner),
            (None, (far, "a"), partner),
            (None, (far, "b"), partner),
        ][kind]
        there = rows(u, *rows_of)
        return pltpu.make_async_remote_copy(
            src_ref=there if source is None else source,
            dst_ref=there,
            send_sem=send.at[u, kind],
            recv_sem=recv.at[u, kind],
            device_id={"dp": to},
            device_id_type=MESH,
        )

    def keep(u):
        return pltpu.make_async_copy(own(u, "all"), rows(u, me, "all"), local.at[u])

    def post(u):
        for kind in (0, 2, 1, 3, 6):
            move(u, kind).start()
        keep(u).start()

    def pass_on(arrived, onward):
        def act(u):
            for one, other in zip(arrived, onward):
                move(u, one).wait_recv()
                move(u, other).start()

        return act

    middle, relay, relay_far = pass_on((0, 2), (4, 5)), pass_on((1, 3), (7, 8)), pass_on((4, 5), (9, 10))

    def finish(u):
        for kind in (6, 7, 8, 9, 10):
            move(u, kind).wait_recv()
        keep(u).wait()

    def both(act, pair):
        act(4 + 2 * pair)
        act(5 + 2 * pair)

    bn, sub = 256, 256

    def when(step, plan):
        for number, act in plan.items():
            pl.when(step == number)(act)

    def first_layer(plan):
        def body(g_ref, u_ref, ku_ref, kg_ref, h_ref):
            when(pl.program_id(0), plan)
            for r in range(0, tokens, sub):
                here = pl.ds(r, sub)
                gate = jnp.dot(a0[here, :], g_ref[...], preferred_element_type=F32)
                up = jnp.dot(a0[here, :], u_ref[...], preferred_element_type=F32)
                sig = 0.5 * jnp.tanh(0.5 * gate) + 0.5
                silu = gate * sig
                ku_ref[here, :] = silu
                kg_ref[here, :] = up * (sig + silu * (1 - sig))
                h_ref[here, :] = (silu * up).astype(BF16)

        w, tile = pl.BlockSpec((d, bn), lambda j: (0, j)), pl.BlockSpec((tokens, bn), lambda j: (0, j))
        pltpu.emit_pipeline(body, grid=(ff // bn,), in_specs=[w, w], out_specs=[tile] * 3)(
            wg.at[0], wu.at[0], keep_up, keep_gate, hid0
        )

    def last_layer(before, after):
        def body(g_ref, u_ref, d_ref, h_ref, bg_ref, bu_ref):
            when(pl.program_id(0), before)
            for r in range(0, tokens, sub):
                here = pl.ds(r, sub)
                gate = jnp.dot(a1[here, :], g_ref[...], preferred_element_type=F32)
                up = jnp.dot(a1[here, :], u_ref[...], preferred_element_type=F32)
                by = mm(dy_ref[here, :], d_ref[...], NT).astype(BF16).astype(F32)
                sig = 0.5 * jnp.tanh(0.5 * gate) + 0.5
                silu = gate * sig
                h_ref[here, :] = (silu * up).astype(BF16)
                bu_ref[here, :] = (by * silu).astype(BF16)
                bg_ref[here, :] = (by * (up * (sig + silu * (1 - sig)))).astype(BF16)
            when(pl.program_id(0), after)

        w, wt = pl.BlockSpec((d, bn), lambda j: (0, j)), pl.BlockSpec((bn, d), lambda j: (j, 0))
        tile = pl.BlockSpec((tokens, bn), lambda j: (0, j))
        pltpu.emit_pipeline(body, grid=(ff // bn,), in_specs=[w, w, wt], out_specs=[tile] * 3)(
            wg.at[1], wu.at[1], wd.at[1], hid1, by_gate, by_up
        )

    rm = 256

    def down(plan):
        def body(hid_ref):
            i = pl.program_id(0)
            when(i, plan)
            here = pl.ds(pl.multiple_of(i * rm, rm), rm)
            out = jnp.dot(hid_ref[...], wd_v[...], preferred_element_type=F32).astype(BF16)
            h = (x_ref[here, :].astype(F32) + out.astype(F32)).astype(BF16)
            h1[here, :] = h
            a = normed(h)
            a1[here, :] = a
            a1t[:, here] = a.T

        pltpu.emit_pipeline(body, grid=(tokens // rm,), in_specs=[pl.BlockSpec((rm, ff), lambda i: (i, 0))], out_specs=[])(hid0)

    def run(*acts):
        def act():
            for f, u in acts:
                f(u)

        return act

    post(0)
    post(1)
    get = pltpu.make_async_copy(dy, dy_ref, load)
    get.start()
    get.wait()

    @pl.loop(0, tokens // rm)
    def _(i):
        here = pl.ds(pl.multiple_of(i * rm, rm), rm)
        a = normed(x_ref[here, :])
        a0[here, :] = a
        a0t[:, here] = a.T

    leaving = [pltpu.make_async_copy(one, out, leave.at[i]) for i, (one, out) in enumerate(((a0t, a0t_out), (h1, h1_out), (a1t, a1t_out)))]
    leaving[0].start()

    def on(p, *acts):
        def act():
            for f in acts:
                both(f, p)

        return act

    run((middle, 0), (relay, 0), (middle, 1), (post, 2), (relay, 1), (relay_far, 0), (relay_far, 1), (finish, 0), (finish, 1))()

    def first_piece():
        middle(3)
        on(0, post)()

    first_layer({5: run((middle, 2), (post, 3)), 10: run((relay, 2)), 16: run((relay_far, 2)), 21: first_piece})
    finish(2)
    get = pltpu.make_async_copy(wd.at[0], wd_v, load)
    get.start()
    get.wait()

    def second_piece():
        on(0, middle)()
        on(1, post)()

    down({0: run((relay, 3)), 4: run((relay_far, 3)), 7: second_piece})
    finish(3)
    on(0, relay, relay_far, finish)()
    leaving[1].start()
    leaving[2].start()
    steps = piece // bn
    before, after = {}, {}

    def advance(p):
        def act():
            on(p, middle)()
            if p + 1 < pieces:
                on(p + 1, post)()

        return act

    for p in range(1, pieces):
        before[steps * p - 4] = advance(p)
        before[steps * p - 3] = on(p, relay)
        before[steps * p - 2] = on(p, relay_far)
        after[steps * p - 2] = on(p, finish)
    last_layer(before, after)
    for one in leaving:
        one.wait()
    for u in range(len(units)):
        for kind in range(11):
            move(u, kind).wait_send()


def forward(n, x, dy, sg, su, sd):
    tokens, d = x.shape
    ff = sg.shape[-1]
    layers = sg.shape[0]
    vmem, hbm = pl.BlockSpec(memory_space=pltpu.VMEM), pl.BlockSpec(memory_space=pl.ANY)
    s = jax.ShapeDtypeStruct
    wide, thin = s((tokens, ff), F32), s((tokens, ff), BF16)
    units, kinds = 16, 11
    return pl.pallas_call(
        functools.partial(forward_kernel, n),
        out_shape=(
            s((layers, d, ff), BF16), s((layers, d, ff), BF16), s((layers, ff, d), BF16),
            wide, wide, thin, thin, thin, thin, s((tokens, d), BF16), s((d, tokens), BF16), s((d, tokens), BF16),
        ),
        in_specs=[vmem] + [hbm] * 4,
        out_specs=[hbm] * 12,
        scratch_shapes=[
            pltpu.VMEM((tokens, d), BF16),
            pltpu.VMEM((d, tokens), BF16),
            pltpu.VMEM((d, tokens), BF16),
            pltpu.VMEM((tokens, d), BF16),
            pltpu.VMEM((tokens, d), BF16),
            pltpu.VMEM((tokens, d), BF16),
            pltpu.VMEM((ff, d), BF16),
            pltpu.SemaphoreType.DMA((units, kinds)),
            pltpu.SemaphoreType.DMA((units, kinds)),
            pltpu.SemaphoreType.DMA((units,)),
            pltpu.SemaphoreType.DMA,
            pltpu.SemaphoreType.DMA((3,)),
        ],
        compiler_params=pltpu.CompilerParams(collective_id=0, has_side_effects=True, vmem_limit_bytes=63 * 1024 * 1024),
        name="forward",
    )(x, dy, sg, su, sd)


def through_norm_kernel(h_ref, by_ref, wg, wu, by_gate, by_up, out, wg_v, wu_v, load):
    tokens, _ = h_ref.shape
    ff = by_gate.shape[1]
    rm = 256
    gets = [pltpu.make_async_copy(w.at[1], w_v, load.at[i]) for i, (w, w_v) in enumerate(((wg, wg_v), (wu, wu_v)))]
    for get in gets:
        get.start()
    for get in gets:
        get.wait()

    def body(bg_ref, bu_ref):
        here = pl.ds(pl.multiple_of(pl.program_id(0) * rm, rm), rm)
        by_a = mm(bg_ref[...], wg_v[...], NT).astype(BF16).astype(F32) + mm(bu_ref[...], wu_v[...], NT).astype(BF16).astype(F32)
        added = normed_back(h_ref[here, :], by_a.astype(BF16))
        out[here, :] = (by_ref[here, :].astype(F32) + added.astype(F32)).astype(BF16)

    rows = pl.BlockSpec((rm, ff), lambda i: (i, 0))
    pltpu.emit_pipeline(body, grid=(tokens // rm,), in_specs=[rows, rows], out_specs=[])(by_gate, by_up)


def through_norm(h, by_h, wg, wu, by_gate, by_up):
    tokens, d = h.shape
    ff = by_gate.shape[1]
    vmem, hbm = pl.BlockSpec(memory_space=pltpu.VMEM), pl.BlockSpec(memory_space=pl.ANY)
    return pl.pallas_call(
        through_norm_kernel,
        out_shape=jax.ShapeDtypeStruct((tokens, d), BF16),
        in_specs=[vmem] * 2 + [hbm] * 4,
        out_specs=vmem,
        scratch_shapes=[pltpu.VMEM((d, ff), BF16)] * 2 + [pltpu.SemaphoreType.DMA((2,))],
        compiler_params=pltpu.CompilerParams(vmem_limit_bytes=62 * 1024 * 1024),
        cost_estimate=pl.CostEstimate(flops=4 * tokens * d * ff, bytes_accessed=4 * (tokens + d) * ff, transcendentals=0),
        name="through_norm",
    )(h, by_h, wg, wu, by_gate, by_up)


def by_weight(a_t, by, start, size):
    d, tokens = a_t.shape
    bn = 1024

    def kernel(a_ref, by_ref, out_ref):
        out_ref[...] = jnp.dot(a_ref[...], by_ref[...], preferred_element_type=F32).astype(BF16)

    return pl.pallas_call(
        kernel,
        out_shape=jax.ShapeDtypeStruct((d, size), BF16),
        grid=(size // bn,),
        in_specs=[pl.BlockSpec((d, tokens), lambda j: (0, 0)), pl.BlockSpec((tokens, bn), lambda j: (0, start // bn + j))],
        out_specs=pl.BlockSpec((d, bn), lambda j: (0, j)),
        compiler_params=pltpu.CompilerParams(vmem_limit_bytes=48 * 1024 * 1024),
        cost_estimate=pl.CostEstimate(flops=2 * d * tokens * size, bytes_accessed=2 * (d + tokens) * size, transcendentals=0),
        name="by_weight",
    )(a_t, by)


def tail_kernel(n, by_ref, at_ref, wd, keep_up, keep_gate, out_gate, out_up, bg, bu, term, there, own, hold, first, second, far_a, far_b, low, high, send, recv):
    me = lax.axis_index("dp")
    chip, core = me // 2, lax.rem(me, 2)
    ring = n // 2
    at = lambda c, k: 2 * lax.rem(c, ring) + k
    right, left, partner = at(chip + 1, core), at(chip + ring - 1, core), at(chip, 1 - core)

    barrier = pltpu.get_barrier_semaphore()
    for other in (left, right, partner):
        pl.semaphore_signal(barrier, inc=1, device_id={"dp": other}, device_id_type=MESH)
    pl.semaphore_wait(barrier, 3)

    tokens, d = by_ref.shape
    slices, bn = there.shape[0], there.shape[-1]
    slots = hold.shape[0]

    def move(u, kind):
        slot = lax.rem(u, slots)
        source, target, to = [
            (term.at[lax.rem(u, 2), :, :, 1 - core], there.at[u], partner),
            (first.at[slot, 0], far_a.at[u], right),
            (first.at[slot, 1], far_b.at[u], left),
            (first.at[slot, 2], low.at[u, 1], right),
            (first.at[slot, 3], high.at[u, 0], left),
            (second.at[slot, 0], low.at[u, 0], right),
            (second.at[slot, 1], high.at[u, 1], left),
        ][kind]
        return pltpu.make_async_remote_copy(
            src_ref=source, dst_ref=target, send_sem=send.at[u, kind], recv_sem=recv.at[u, kind], device_id={"dp": to}, device_id_type=MESH
        )

    def pair_sum(u):
        slot, turn = lax.rem(u, slots), lax.rem(u, 2)
        move(u, 0).wait_recv()

        @pl.when(u >= slots)
        def _():
            for kind in (1, 2, 3, 4):
                move(u - slots, kind).wait_send()

        def both(away, which):
            c = lax.rem(chip + away, ring)
            return term[turn, which, c, core].astype(F32) + there[u, which, c].astype(F32)

        for i, (away, which) in enumerate(((2, 0), (2, 1), (1, 1), (ring - 1, 0))):
            first[slot, i] = both(away, which).astype(BF16)
        for kind in (1, 2, 3, 4):
            move(u, kind).start()
        hold[slot, 0] = both(1, 0)
        hold[slot, 1] = both(ring - 1, 1)
        for which in range(2):
            own[u, which] = both(0, which)

    def add_far(u):
        slot = lax.rem(u, slots)

        @pl.when(u >= slots)
        def _():
            for kind in (5, 6):
                move(u - slots, kind).wait_send()

        for i, far in enumerate((far_a, far_b)):
            move(u, 1 + i).wait_recv()
            second[slot, i] = (hold[slot, i] + far[u].astype(F32)).astype(BF16)
            move(u, 5 + i).start()

    def finish(u):
        for kind in (3, 4, 5, 6):
            move(u, kind).wait_recv()
        columns = pl.ds(pl.multiple_of(u * bn, bn), bn)
        for which, out in enumerate((out_gate, out_up)):
            total = own[u, which] + low[u, which].astype(F32) + high[u, which].astype(F32)
            out[:, columns] = total.astype(BF16)

    bm, sub = tokens // 2, 256

    def body(d_ref, ku_ref, kg_ref):
        j, i = pl.program_id(0), pl.program_id(1)

        @pl.when((i == 0) & (j >= 3))
        def _():
            finish(j - 3)

        @pl.when((i == 0) & (j >= 2))
        def _():
            add_far(j - 2)

        for r in range(0, bm, sub):
            here, whole = pl.ds(r, sub), pl.ds(pl.multiple_of(i * bm + r, sub), sub)
            by = mm(by_ref[whole, :], d_ref[...], NT).astype(BF16).astype(F32)
            bu[whole, :] = (by * ku_ref[here, :]).astype(BF16)
            bg[whole, :] = (by * kg_ref[here, :]).astype(BF16)

        @pl.when((i == 0) & (j >= 1))
        def _():
            pair_sum(j - 1)

        @pl.when(i == 1)
        def _():
            @pl.when(j >= 2)
            def _():
                move(j - 2, 0).wait_send()

            for which, by in enumerate((bg, bu)):
                g = jnp.dot(at_ref[...], by[...], preferred_element_type=F32).astype(BF16)
                term[lax.rem(j, 2), which] = g.reshape(term.shape[2:])
            move(j, 0).start()

    tile = pl.BlockSpec((bm, bn), lambda j, i: (i, j))
    pltpu.emit_pipeline(
        body, grid=(slices, 2), in_specs=[pl.BlockSpec((bn, d), lambda j, i: (j, 0)), tile, tile], out_specs=[]
    )(wd.at[0], keep_up, keep_gate)

    finish(slices - 3)
    add_far(slices - 2)
    pair_sum(slices - 1)
    finish(slices - 2)
    add_far(slices - 1)
    finish(slices - 1)
    for u in range(slices - 2, slices):
        move(u, 0).wait_send()
    for u in range(slices - slots, slices):
        for kind in range(1, 7):
            move(u, kind).wait_send()


def tail(n, by_h, a_t, wd, keep_up, keep_gate):
    tokens, d = by_h.shape
    ff = keep_up.shape[1]
    depth, bn = d // n, 512
    slices, slots, ring = ff // bn, 4, n // 2
    vmem, hbm = pl.BlockSpec(memory_space=pltpu.VMEM), pl.BlockSpec(memory_space=pl.ANY)
    block = (depth, bn)
    return pl.pallas_call(
        functools.partial(tail_kernel, n),
        out_shape=(jax.ShapeDtypeStruct((depth, ff), BF16),) * 2,
        in_specs=[vmem, vmem, hbm, hbm, hbm],
        out_specs=(vmem, vmem),
        scratch_shapes=[
            pltpu.VMEM((tokens, bn), BF16),
            pltpu.VMEM((tokens, bn), BF16),
            pltpu.VMEM((2, 2, ring, 2) + block, BF16),
            pltpu.VMEM((slices, 2, ring) + block, BF16),
            pltpu.VMEM((slices, 2) + block, F32),
            pltpu.VMEM((slots, 2) + block, F32),
            pltpu.VMEM((slots, 4) + block, BF16),
            pltpu.VMEM((slots, 2) + block, BF16),
            pltpu.VMEM((slices,) + block, BF16),
            pltpu.VMEM((slices,) + block, BF16),
            pltpu.VMEM((slices, 2) + block, BF16),
            pltpu.VMEM((slices, 2) + block, BF16),
            pltpu.SemaphoreType.DMA((slices, 7)),
            pltpu.SemaphoreType.DMA((slices, 7)),
        ],
        compiler_params=pltpu.CompilerParams(collective_id=1, has_side_effects=True, vmem_limit_bytes=63 * 1024 * 1024),
        name="tail",
    )(by_h, a_t, wd, keep_up, keep_gate)


def adamw(w, m, v, g):
    m = 0.9 * m + 0.1 * g
    v = 0.95 * v + 0.05 * g * g
    step = m * lax.rsqrt(v + 1e-8) + 0.1 * w
    return (w - 0.02 * step).astype(BF16), m, v


def solution(mesh):
    n = mesh.shape["dp"]

    def scatter(g):
        return lax.psum_scatter(g, "dp", scatter_dimension=0, tiled=True)

    def inner(x, dy, *arrays):
        weights, m, v = (arrays[i : i + 3] for i in (0, 3, 6))
        layers = weights[0].shape[0]
        wg, wu, wd, keep_up, keep_gate, hid0, hid1, by_gate, by_up, h1, a1t, a0t = forward(n, x[0], dy[0], *weights)
        by_h = dy[0]
        ff = by_gate.shape[1]
        g_gate = by_weight(a1t, by_gate, 0, ff)
        r1 = scatter(g_gate)
        hid1, g_gate = lax.optimization_barrier((hid1, g_gate))
        g_down = mm(hid1, by_h, TN).astype(BF16)
        r0 = scatter(g_down)
        by_up, g_down = lax.optimization_barrier((by_up, g_down))
        g_up = by_weight(a1t, by_up, 0, ff)
        r2 = scatter(g_up)
        by_gate, by_up, g_up = lax.optimization_barrier((by_gate, by_up, g_up))
        by_h = through_norm(h1, by_h, wg, wu, by_gate, by_up)
        g_down = mm(hid0, by_h, TN).astype(BF16)
        r3 = scatter(g_down)
        by_h, g_down = lax.optimization_barrier((by_h, g_down))
        r4, r5 = tail(n, by_h, a0t, wd, keep_up, keep_gate)
        mine = [[r4, r5, r3], [r1, r2, r0]]
        new = []
        for i in range(3):
            g = jnp.stack([mine[layer][i] for layer in range(layers)]).astype(F32)
            new.append(adamw(weights[i].astype(F32), m[i], v[i], g))
        return tuple(one[which] for which in range(3) for one in new)

    states, cut = P(("rep", "dp"), None, None), P(None, "dp", None)
    return jax.shard_map(
        inner,
        mesh=mesh,
        in_specs=(states, states) + (cut,) * 9,
        out_specs=(P("rep", "dp", None),) * 9,
        check_vma=False,
    )
```
